32 devices in a mesh: row: 8 (over z, y), col: 4 (over x, core).
Axes of the slice: x: 2, y: 2, z: 4, core: 2. Of those that a mesh axis runs over, the one named last changes fastest.
Arguments:
- tracer: float32 [128, 128, 512], P(None, 'row', 'col'), may hold values from -6 to 6
- symbol_x: float32 [128], replicated, may hold values from 0.3 to 3
- symbol_y: float32 [128], replicated, may hold values from 0.3 to 3
- symbol_z: float32 [512], replicated, may hold values from 0.3 to 3
Outputs:
- spectrum: float32 [128, 128, 512], P('row', 'col')
The draws below stay inside these ranges and needn't reach their ends.
All inputs are finite; a program needn't handle non-finite values.
Results may differ from the reference program's by a relative error of at most 0.000075.
Values sent between devices are 32-bit elements; how exact they have to be, the bound alone decides.
A program may use at most 64 MiB of HBM per device.

```python
import jax
import jax.numpy as jnp
from jax import lax

GRID_X = 128
GRID_Y = 128
GRID_Z = 512


def level_of(stream_key, extent, shards, smallest, largest):
    def one(axis_at, shards_of):
        draws = jax.random.uniform(jax.random.fold_in(jax.random.fold_in(stream_key, 6), axis_at), (shards_of,), jnp.float32, smallest / len(shards), largest / len(shards))
        return jnp.repeat(jnp.exp(draws), extent[axis_at] // shards_of).reshape((-1,) + (1,) * (len(extent) - axis_at - 1))

    level = one(*shards[0])
    for cut in shards[1:]:
        level = level * one(*cut)
    return level


def gaussian(key, dims, deviation, most, cuts=(), dtype=jnp.bfloat16):
    loudness = level_of(key, dims, cuts, -0.22, 0.18) if cuts else 1.0
    values = jax.random.normal(key, dims, jnp.float32) * deviation * loudness
    return jnp.minimum(jnp.maximum(values, -most), most).astype(dtype)


def setup_inputs(seed: int = 0) -> dict:
    seeds = jax.random.split(jax.random.key(seed), 5)
    return {
        "tracer": gaussian(seeds[0], (GRID_X, GRID_Y, GRID_Z), 1.0, 6.0, ((1, 8), (2, 4)), jnp.float32),
        "symbol_x": jnp.clip(jax.random.uniform(seeds[1], (GRID_X,), jnp.float32, 0.3, 3.0), 0.3, 3.0),
        "symbol_y": jnp.clip(jax.random.uniform(seeds[2], (GRID_Y,), jnp.float32, 0.3, 3.0), 0.3, 3.0),
        "symbol_z": jnp.clip(jax.random.uniform(seeds[3], (GRID_Z,), jnp.float32, 0.3, 3.0), 0.3, 3.0),
    }


def transform_table(count):
    rank = jnp.arange(count)
    angle = (jnp.pi / (count + 1)) * (((rank[:, None] + 1) * (rank[None, :] + 1)) % (2 * count + 2)).astype(jnp.float32)
    return jnp.sin(angle) * (2.0 / (count + 1)) ** 0.5


def to_modes(values, dim):
    moved = jnp.tensordot(values, transform_table(values.shape[dim]), axes=([dim], [0]), precision=lax.Precision.HIGHEST)
    return jnp.moveaxis(moved, -1, dim)


def reference(tracer, symbol_x, symbol_y, symbol_z):
    spectrum = tracer
    spectrum = to_modes(spectrum, 0)
    spectrum = to_modes(spectrum, 1)
    spectrum = to_modes(spectrum, 2)
    symbol = symbol_x[:, None, None] + symbol_y[None, :, None] + symbol_z[None, None, :]
    spectrum = spectrum * ((1.0 - 0.2 * symbol) / (1.0 + 0.2 * symbol))
    return spectrum
```

```python
import functools

import jax
import jax.numpy as jnp
import ml_dtypes
import numpy as np
from jax import lax
from jax.experimental import pallas as pl
from jax.experimental.pallas import tpu as pltpu
from jax.sharding import PartitionSpec as P

MESH = pl.DeviceIdType.MESH
F32 = jnp.float32
BF16 = jnp.bfloat16
PIECES = 8


def table_halves(count):
    rank = np.arange(1, count + 1)
    turns = np.outer(rank, rank) % (2 * count + 2)
    table = np.sin(np.pi / (count + 1) * turns) * np.sqrt(2.0 / (count + 1))
    high = table.astype(ml_dtypes.bfloat16)
    low = (table - high.astype(np.float64)).astype(ml_dtypes.bfloat16)
    return high, low


def halves(values):
    high = values.astype(BF16)
    return high, (values - high.astype(F32)).astype(BF16)


def dot(a, b):
    return jnp.dot(a, b, preferred_element_type=F32)


def from_left(stacked, values):
    rows = stacked.shape[0] // 2
    high, low = halves(values)
    both = dot(stacked, high)
    return both[:rows] + both[rows:] + dot(stacked[:rows], low)


def kernel(
    n, m, pieces, groups, block,
    field, tab_x, tab_y, tab_zh, tab_zl, sx, sy, sz, out,
    d, s, r, y, c, f, o, tx, ty, tzh, tzl, colx, coly, vx, vy, vz,
    in_sem, tab_sem, send_r, recv_r, send_c, recv_c, out_sem,
):
    me_r, me_c = lax.axis_index("row"), lax.axis_index("col")
    depth, ys, zs = d.shape
    each = r.shape[0] // pieces
    per = n * each
    yc = y.shape[3]
    loads = [(field, d, 0), (tab_x, tx, 1), (tab_y, ty, 2), (tab_zh, tzh, 3), (tab_zl, tzl, 4)]
    loads += [(sx, vx, 5), (sy, vy, 6), (sz, vz, 7)]
    loads = [pltpu.make_async_copy(a, b, in_sem.at[i]) for a, b, i in loads]
    for load in loads:
        load.start()

    barrier = pltpu.get_barrier_semaphore()

    def greet(axis, me, size):
        def one(i, _):
            pl.semaphore_signal(
                barrier, inc=1, device_id={axis: lax.rem(me + i, size)}, device_id_type=MESH
            )
            return 0

        lax.fori_loop(1, size, one, 0)

    greet("row", me_r, n)
    greet("col", me_c, m)

    loads[0].wait()
    loads[1].wait()
    lanes = d.reshape(depth * ys, zs)
    modes = s.reshape(s.shape[0] * ys, zs)

    def transform_x(first, count):
        rows = count * per
        stacked = tx[2 * first * per : 2 * (first + count) * per]

        def pair(i, _):
            got = jnp.concatenate(
                [lanes[pl.ds(2 * i + h, depth, stride=ys), :] for h in range(2)], axis=1
            )
            got = from_left(stacked, got)
            for h in range(2):
                modes[pl.ds(first * per * ys + 2 * i + h, rows, stride=ys), :] = got[
                    :, h * zs : (h + 1) * zs
                ]
            return 0

        lax.fori_loop(0, ys // 2, pair, 0, unroll=True)

    def send_rows(k):
        def one(i, _):
            step = n // 2 + (i + 1) // 2 * (2 * (i % 2) - 1)
            to = lax.rem(me_r + step, n)
            pltpu.make_async_remote_copy(
                src_ref=s.at[pl.ds(k * per + to * each, each)],
                dst_ref=r.at[pl.ds(k * each, each), pl.ds(pl.multiple_of(me_r * ys, ys), ys), :],
                send_sem=send_r.at[k],
                recv_sem=recv_r.at[k],
                device_id={"row": to},
                device_id_type=MESH,
            ).start()
            return 0

        lax.fori_loop(0, n - 1, one, 0)
        r[pl.ds(k * each, each), pl.ds(pl.multiple_of(me_r * ys, ys), ys), :] = s[
            pl.ds(k * per + me_r * each, each)
        ]

    for at, (first, count) in enumerate(groups):
        transform_x(first, count)
        if at == 0:
            pl.semaphore_wait(barrier, n + m - 2)
        for k in range(first, first + count):
            send_rows(k)

    for load in loads[2:]:
        load.wait()

    def upright(row_ref, into):
        size = row_ref.shape[1]
        here = lax.broadcasted_iota(jnp.int32, (size, size), 0)
        there = lax.broadcasted_iota(jnp.int32, (size, size), 1)
        kept = jnp.where(here == there, row_ref[...], 0.0)
        into[...] = jnp.broadcast_to(jnp.sum(kept, axis=1, keepdims=True), into.shape)

    upright(vx, colx)
    upright(vy, coly)
    x_share = r.shape[0]
    part_y = coly[pl.ds(pl.multiple_of(me_c * yc, yc), yc), :]

    def factor(i, _):
        symbol = part_y + colx[pl.ds(me_r * x_share + i, 1), :]
        for at in range(0, vz.shape[1], 128):
            full = symbol + vz[:, at : at + 128]
            f[pl.ds(pl.multiple_of(i * yc, yc), yc), at : at + 128] = (1.0 - 0.2 * full) / (
                1.0 + 0.2 * full
            )
        return 0

    lax.fori_loop(0, x_share, factor, 0)

    def got_rows(k):
        waited = r.at[pl.ds(k * each, each), pl.ds(0, (n - 1) * ys), :]
        pltpu.make_async_copy(waited, waited, recv_r.at[k]).wait()

    def transform_y(k):
        got = jnp.concatenate([r[k * each + j] for j in range(each)], axis=1)
        for b in range(ty.shape[0] // (2 * block)):
            now = from_left(ty[2 * b * block : 2 * (b + 1) * block], got)
            for q in range(block // yc):
                for j in range(each):
                    y[k, b * (block // yc) + q, j] = now[
                        q * yc : (q + 1) * yc, j * zs : (j + 1) * zs
                    ]

    def send_cols(k):
        def one(i, _):
            to = lax.rem(me_c + i, m)
            pltpu.make_async_remote_copy(
                src_ref=y.at[k, to],
                dst_ref=c.at[k, me_c],
                send_sem=send_c.at[k],
                recv_sem=recv_c.at[k],
                device_id={"col": to},
                device_id_type=MESH,
            ).start()
            return 0

        lax.fori_loop(1, m, one, 0)
        c[k, me_c] = y[k, me_c]

    def got_cols(k):
        waited = c.at[k, pl.ds(0, m - 1)]
        pltpu.make_async_copy(waited, waited, recv_c.at[k]).wait()

    def written(k):
        rows = pl.ds(pl.multiple_of(k * each * yc, each * yc), each * yc)
        return pltpu.make_async_copy(o.at[rows, :], out.at[rows, :], out_sem.at[k])

    def transform_z(k):
        rows = each * yc
        got = jnp.concatenate([c[k, q].reshape(rows, zs) for q in range(m)], axis=1)
        high, low = halves(got)
        both = dot(jnp.concatenate([high, low], axis=0), tzh[...])
        full = both[:rows] + both[rows:] + dot(high, tzl[...])
        at = pl.ds(pl.multiple_of(k * rows, rows), rows)
        o[at, :] = full * f[at, :]
        written(k).start()

    def step(k, _):
        got_rows(k)
        transform_y(k)
        send_cols(k)

        @pl.when(k > 0)
        def _():
            got_cols(k - 1)
            transform_z(k - 1)

        return 0

    lax.fori_loop(0, pieces, step, 0)
    got_cols(pieces - 1)
    transform_z(pieces - 1)

    def finish(k, _):
        sent = s.at[pl.ds(0, (n - 1) * each)]
        pltpu.make_async_copy(sent, sent, send_r.at[k]).wait()
        sent = y.at[k, pl.ds(0, m - 1)]
        pltpu.make_async_copy(sent, sent, send_c.at[k]).wait()
        written(k).wait()
        return 0

    lax.fori_loop(0, pieces, finish, 0)


def per_device(n, m, tracer, symbol_x, symbol_y, symbol_z):
    depth, ys, zs = tracer.shape
    height, length = ys * n, zs * m
    x_share, yc = depth // n, height // m
    pieces = min(PIECES, x_share)
    each = x_share // pieces
    per = n * each
    block = min(height, 128)

    groups = [(0, 1)]
    most = max(1, 128 // per)
    while sum(groups[-1]) < pieces:
        first = sum(groups[-1])
        groups.append((first, min(most, pieces - first)))
    order = np.arange(depth).reshape(n, pieces, each).transpose(1, 0, 2).reshape(pieces, per)
    high, low = table_halves(depth)
    tab_x = []
    for first, count in groups:
        rows = order[first : first + count].reshape(-1)
        tab_x += [high[rows], low[rows]]
    tab_x = np.concatenate(tab_x)
    high, low = table_halves(height)
    tab_y = []
    for b in range(0, height, block):
        tab_y += [high[b : b + block], low[b : b + block]]
    tab_y = np.concatenate(tab_y)
    tab_zh, tab_zl = table_halves(length)

    anywhere = pl.BlockSpec(memory_space=pl.ANY)
    dma = pltpu.SemaphoreType.DMA
    out = pl.pallas_call(
        functools.partial(kernel, n, m, pieces, groups, block),
        out_shape=jax.ShapeDtypeStruct((x_share * yc, length), F32),
        in_specs=[anywhere] * 8,
        out_specs=anywhere,
        scratch_shapes=[
            pltpu.VMEM((depth, ys, zs), F32),
            pltpu.VMEM((depth, ys, zs), F32),
            pltpu.VMEM((x_share, height, zs), F32),
            pltpu.VMEM((pieces, m, each, yc, zs), F32),
            pltpu.VMEM((pieces, m, each, yc, zs), F32),
            pltpu.VMEM((x_share * yc, length), F32),
            pltpu.VMEM((x_share * yc, length), F32),
            pltpu.VMEM(tab_x.shape, BF16),
            pltpu.VMEM(tab_y.shape, BF16),
            pltpu.VMEM(tab_zh.shape, BF16),
            pltpu.VMEM(tab_zl.shape, BF16),
            pltpu.VMEM((depth, 128), F32),
            pltpu.VMEM((height, 128), F32),
            pltpu.VMEM((1, depth), F32),
            pltpu.VMEM((1, height), F32),
            pltpu.VMEM((1, length), F32),
            dma((8,)),
            dma((1,)),
            dma((pieces,)),
            dma((pieces,)),
            dma((pieces,)),
            dma((pieces,)),
            dma((pieces,)),
        ],
        compiler_params=pltpu.CompilerParams(collective_id=0, has_side_effects=True),
    )(
        tracer,
        jnp.asarray(tab_x),
        jnp.asarray(tab_y),
        jnp.asarray(tab_zh),
        jnp.asarray(tab_zl),
        symbol_x[None],
        symbol_y[None],
        symbol_z[None],
    )
    return out.reshape(x_share, yc, length)


def solution(mesh):
    in_specs = (P(None, "row", "col"), P(), P(), P())
    out_specs = P("row", "col", None)
    body = functools.partial(per_device, mesh.shape["row"], mesh.shape["col"])
    return jax.shard_map(
        body, mesh=mesh, in_specs=in_specs, out_specs=out_specs, check_vma=False
    )
```

```python
import functools

import jax
import jax.numpy as jnp
import ml_dtypes
import numpy as np
from jax import lax
from jax.experimental import pallas as pl
from jax.experimental.pallas import tpu as pltpu
from jax.sharding import PartitionSpec as P

MESH = pl.DeviceIdType.MESH
F32 = jnp.float32
BF16 = jnp.bfloat16
PIECES = 4
LAG = 1


def table_halves(count):
    rank = np.arange(1, count + 1)
    turns = np.outer(rank, rank) % (2 * count + 2)
    table = np.sin(np.pi / (count + 1) * turns) * np.sqrt(2.0 / (count + 1))
    high = table.astype(ml_dtypes.bfloat16)
    low = (table - high.astype(np.float64)).astype(ml_dtypes.bfloat16)
    return high, low


def halves(values):
    high = values.astype(BF16)
    return high, (values - high.astype(F32)).astype(BF16)


def dot(a, b):
    return jnp.dot(a, b, preferred_element_type=F32)


def from_left(stacked, values):
    rows = stacked.shape[0] // 2
    high, low = halves(values)
    both = dot(stacked, high)
    return both[:rows] + both[rows:] + dot(stacked[:rows], low)


def kernel(
    n, m, pieces, groups, block,
    field, tab_x, tab_y, tab_zh, tab_zl, sx, sy, sz, out,
    d, s, r, y, c, f, tx, ty, tzh, tzl, colx, coly, vx, vy, vz,
    in_sem, tab_sem, send_r, recv_r, send_c, recv_c,
):
    lag = min(LAG, pieces)
    me_r, me_c = lax.axis_index("row"), lax.axis_index("col")
    depth, ys, zs = d.shape
    each = r.shape[0] // pieces
    per = n * each
    yc = y.shape[3]
    loads = [(field, d, 0), (tab_x, tx, 1), (tab_y, ty, 2), (tab_zh, tzh, 3), (tab_zl, tzl, 4)]
    loads += [(sx, vx, 5), (sy, vy, 6), (sz, vz, 7)]
    loads = [pltpu.make_async_copy(a, b, in_sem.at[i]) for a, b, i in loads]
    for load in loads:
        load.start()

    barrier = pltpu.get_barrier_semaphore()

    def greet(axis, me, size):
        def one(i, _):
            pl.semaphore_signal(
                barrier, inc=1, device_id={axis: lax.rem(me + i, size)}, device_id_type=MESH
            )
            return 0

        lax.fori_loop(1, size, one, 0)

    greet("row", me_r, n)
    greet("col", me_c, m)

    loads[0].wait()
    loads[1].wait()
    lanes = d.reshape(depth * ys, zs)
    modes = s.reshape(s.shape[0] * ys, zs)

    def transform_x(first, count):
        rows = count * per
        stacked = tx[2 * first * per : 2 * (first + count) * per]

        def pair(i, _):
            got = jnp.concatenate(
                [lanes[pl.ds(2 * i + h, depth, stride=ys), :] for h in range(2)], axis=1
            )
            got = from_left(stacked, got)
            for h in range(2):
                modes[pl.ds(first * per * ys + 2 * i + h, rows, stride=ys), :] = got[
                    :, h * zs : (h + 1) * zs
                ]
            return 0

        lax.fori_loop(0, ys // 2, pair, 0, unroll=True)

    def send_rows(k):
        def one(i, _):
            to = lax.rem(me_r + 1 + i, n)
            pltpu.make_async_remote_copy(
                src_ref=s.at[pl.ds(k * per + to * each, each)],
                dst_ref=r.at[pl.ds(k * each, each), pl.ds(pl.multiple_of(me_r * ys, ys), ys), :],
                send_sem=send_r.at[k],
                recv_sem=recv_r.at[k],
                device_id={"row": to},
                device_id_type=MESH,
            ).start()
            return 0

        lax.fori_loop(0, n - 1, one, 0)
        r[pl.ds(k * each, each), pl.ds(pl.multiple_of(me_r * ys, ys), ys), :] = s[
            pl.ds(k * per + me_r * each, each)
        ]

    for at, (first, count) in enumerate(groups):
        transform_x(first, count)
        if at == 0:
            pl.semaphore_wait(barrier, n + m - 2)
        for k in range(first, first + count):
            send_rows(k)

    for load in loads[2:]:
        load.wait()

    def upright(row_ref, into):
        size = row_ref.shape[1]
        here = lax.broadcasted_iota(jnp.int32, (size, size), 0)
        there = lax.broadcasted_iota(jnp.int32, (size, size), 1)
        kept = jnp.where(here == there, row_ref[...], 0.0)
        into[...] = jnp.broadcast_to(jnp.sum(kept, axis=1, keepdims=True), into.shape)

    upright(vx, colx)
    upright(vy, coly)
    x_share = r.shape[0]
    part_y = coly[pl.ds(pl.multiple_of(me_c * yc, yc), yc), :]

    def factor(i, _):
        symbol = part_y + colx[pl.ds(me_r * x_share + i, 1), :]
        for at in range(0, vz.shape[1], 128):
            full = symbol + vz[:, at : at + 128]
            f[pl.ds(pl.multiple_of(i * yc, yc), yc), at : at + 128] = (1.0 - 0.2 * full) / (
                1.0 + 0.2 * full
            )
        return 0

    lax.fori_loop(0, x_share, factor, 0)

    def got_rows(k):
        waited = r.at[pl.ds(k * each, each), pl.ds(0, (n - 1) * ys), :]
        pltpu.make_async_copy(waited, waited, recv_r.at[k]).wait()

    def transform_y(k):
        got = jnp.concatenate([r[k * each + j] for j in range(each)], axis=1)
        for b in range(ty.shape[0] // (2 * block)):
            now = from_left(ty[2 * b * block : 2 * (b + 1) * block], got)
            for q in range(block // yc):
                for j in range(each):
                    y[k, b * (block // yc) + q, j] = now[
                        q * yc : (q + 1) * yc, j * zs : (j + 1) * zs
                    ]

    def send_cols(k):
        def one(i, _):
            to = lax.rem(me_c + i, m)
            pltpu.make_async_remote_copy(
                src_ref=y.at[k, to],
                dst_ref=c.at[k, me_c],
                send_sem=send_c.at[k],
                recv_sem=recv_c.at[k],
                device_id={"col": to},
                device_id_type=MESH,
            ).start()
            return 0

        lax.fori_loop(1, m, one, 0)
        c[k, me_c] = y[k, me_c]

    def got_cols(k):
        waited = c.at[k, pl.ds(0, m - 1)]
        pltpu.make_async_copy(waited, waited, recv_c.at[k]).wait()

    def transform_z(k):
        rows = each * yc
        got = jnp.concatenate([c[k, q].reshape(rows, zs) for q in range(m)], axis=1)
        high, low = halves(got)
        both = dot(jnp.concatenate([high, low], axis=0), tzh[...])
        full = both[:rows] + both[rows:] + dot(high, tzl[...])
        at = pl.ds(pl.multiple_of(k * rows, rows), rows)
        out[at, :] = full * f[at, :]

    def step(k, _):
        got_rows(k)
        transform_y(k)
        send_cols(k)

        @pl.when(k >= lag)
        def _():
            got_cols(k - lag)
            transform_z(k - lag)

        return 0

    lax.fori_loop(0, pieces, step, 0)
    def drain(k, _):
        got_cols(k)
        transform_z(k)
        return 0

    lax.fori_loop(pieces - lag, pieces, drain, 0)

    def finish(k, _):
        sent = s.at[pl.ds(0, (n - 1) * each)]
        pltpu.make_async_copy(sent, sent, send_r.at[k]).wait()
        sent = y.at[k, pl.ds(0, m - 1)]
        pltpu.make_async_copy(sent, sent, send_c.at[k]).wait()
        return 0

    lax.fori_loop(0, pieces, finish, 0)


def per_device(n, m, tracer, symbol_x, symbol_y, symbol_z):
    depth, ys, zs = tracer.shape
    height, length = ys * n, zs * m
    x_share, yc = depth // n, height // m
    pieces = min(PIECES, x_share)
    each = x_share // pieces
    per = n * each
    block = min(height, 128)

    groups = [(0, 1)]
    most = max(1, 128 // per)
    while sum(groups[-1]) < pieces:
        first = sum(groups[-1])
        groups.append((first, min(most, pieces - first)))
    order = np.arange(depth).reshape(n, pieces, each).transpose(1, 0, 2).reshape(pieces, per)
    high, low = table_halves(depth)
    tab_x = []
    for first, count in groups:
        rows = order[first : first + count].reshape(-1)
        tab_x += [high[rows], low[rows]]
    tab_x = np.concatenate(tab_x)
    high, low = table_halves(height)
    tab_y = []
    for b in range(0, height, block):
        tab_y += [high[b : b + block], low[b : b + block]]
    tab_y = np.concatenate(tab_y)
    tab_zh, tab_zl = table_halves(length)

    anywhere = pl.BlockSpec(memory_space=pl.ANY)
    dma = pltpu.SemaphoreType.DMA
    out = pl.pallas_call(
        functools.partial(kernel, n, m, pieces, groups, block),
        out_shape=pltpu.VMEM((x_share * yc, length), F32),
        in_specs=[anywhere] * 8,
        out_specs=pl.BlockSpec(memory_space=pltpu.VMEM),
        scratch_shapes=[
            pltpu.VMEM((depth, ys, zs), F32),
            pltpu.VMEM((depth, ys, zs), F32),
            pltpu.VMEM((x_share, height, zs), F32),
            pltpu.VMEM((pieces, m, each, yc, zs), F32),
            pltpu.VMEM((pieces, m, each, yc, zs), F32),
            pltpu.VMEM((x_share * yc, length), F32),
            pltpu.VMEM(tab_x.shape, BF16),
            pltpu.VMEM(tab_y.shape, BF16),
            pltpu.VMEM(tab_zh.shape, BF16),
            pltpu.VMEM(tab_zl.shape, BF16),
            pltpu.VMEM((depth, 128), F32),
            pltpu.VMEM((height, 128), F32),
            pltpu.VMEM((1, depth), F32),
            pltpu.VMEM((1, height), F32),
            pltpu.VMEM((1, length), F32),
            dma((8,)),
            dma((1,)),
            dma((pieces,)),
            dma((pieces,)),
            dma((pieces,)),
            dma((pieces,)),
        ],
        compiler_params=pltpu.CompilerParams(
            collective_id=0,
            has_side_effects=True,
            vmem_limit_bytes=(58 << 20) - 12 * x_share * yc * length,
        ),
    )(
        tracer,
        jnp.asarray(tab_x),
        jnp.asarray(tab_y),
        jnp.asarray(tab_zh),
        jnp.asarray(tab_zl),
        symbol_x[None],
        symbol_y[None],
        symbol_z[None],
    )
    return out.reshape(x_share, yc, length)


def solution(mesh):
    in_specs = (P(None, "row", "col"), P(), P(), P())
    out_specs = P("row", "col", None)
    body = functools.partial(per_device, mesh.shape["row"], mesh.shape["col"])
    return jax.shard_map(
        body, mesh=mesh, in_specs=in_specs, out_specs=out_specs, check_vma=False
    )
```
